32 devices in a mesh: row: 8 (over y, x, core), col: 4 (over z).
Axes of the slice: x: 2, y: 2, z: 4, core: 2. Of those that a mesh axis runs over, the one named last changes fastest.
Arguments:
- trailing: bfloat16 [4096, 8192], P('row', 'col'), may hold values from -6 to 6
- col_u: bfloat16 [8, 512, 64], P('row', 'col'), may hold values from -6 to 6
- col_v: bfloat16 [8, 512, 64], P('row', 'col'), may hold values from -0.75 to 0.75
- row_u: bfloat16 [16, 512, 64], P('col', 'row'), may hold values from -6 to 6
- row_v: bfloat16 [16, 512, 64], P('col', 'row'), may hold values from -0.03125 to 0.03125
- diag_lower_inv: float32 [512, 512], replicated, may hold values from -0.176776695 to 1, as said below
- diag_upper_inv: float32 [512, 512], replicated, may hold values from -0.176776695 to 2, as said below
Outputs:
- schur: bfloat16 [4096, 8192], P('row', 'col')
The draws below stay inside these ranges and needn't reach their ends.
Inputs may be any that keep to these rules, and one draw needn't show every extreme that they name: `diag_lower_inv`: lower triangular with unit diagonal. `diag_upper_inv`: upper triangular with diagonal entries between 0.5 and 2.
All inputs are finite; a program needn't handle non-finite values.
Results may differ from the reference program's by a relative error of at most 0.0054.
Values may be sent and summed in bfloat16 or wider, within the bound.
A program may use at most 64 MiB of HBM per device.

```python
import jax
import jax.numpy as jnp
from jax import lax

B = 512
R = 64
MT = 8
NT = 16


def draw_diag_lower_inv(key, part):
    noise = jnp.clip(jax.random.normal(jax.random.fold_in(key, 11), (B, B), jnp.float32), -4.0, 4.0)
    below = jnp.tril(noise, -1) / jnp.sqrt(jnp.float32(B))
    return below + jnp.eye(B, dtype=jnp.float32)


def draw_diag_upper_inv(key, part):
    noise = jnp.clip(jax.random.normal(jax.random.fold_in(key, 23), (B, B), jnp.float32), -4.0, 4.0)
    above = jnp.triu(noise, 1) / jnp.sqrt(jnp.float32(B))
    pivots = jax.random.uniform(jax.random.fold_in(key, 37), (B,), jnp.float32, 0.5, 2.0)
    return above + jnp.diag(pivots)


def level_of(own_key, dims, shards, low, top_value):
    def one(axis_at, blocks):
        steps = jax.random.uniform(jax.random.fold_in(jax.random.fold_in(own_key, 6), axis_at), (blocks,), jnp.float32, low / len(shards), top_value / len(shards))
        return jnp.repeat(jnp.exp(steps), dims[axis_at] // blocks).reshape((-1,) + (1,) * (len(dims) - axis_at - 1))

    gain = one(*shards[0])
    for cut in shards[1:]:
        gain = gain * one(*cut)
    return gain


def normal_values(own_key, dims, scale, limit, pieces=(), kind=jnp.bfloat16):
    values = scale * jax.random.normal(own_key, dims, jnp.float32)
    if pieces:
        values = values * level_of(own_key, dims, pieces, -0.22, 0.18)
    return jnp.clip(values, -limit, limit).astype(kind)


def setup_inputs(seed: int = 0) -> dict:
    key_of = jax.random.split(jax.random.key(seed), 8)
    trailing = normal_values(key_of[0], (MT * B, NT * B), 1.0, 6.0, ((0, 8), (1, 4)))
    col_u = normal_values(key_of[1], (MT, B, R), 1.0, 6.0, ((0, 8), (1, 4)))
    col_v = normal_values(key_of[2], (MT, B, R), R ** -0.5, 0.75, ((0, 8), (1, 4)))
    row_u = normal_values(key_of[3], (NT, B, R), 1.0, 6.0, ((0, 4), (1, 8)))
    row_v = normal_values(key_of[4], (NT, B, R), (R * B) ** -0.5, 0.03125, ((0, 4), (1, 8)))
    diag_lower_inv = draw_diag_lower_inv(jax.random.fold_in(key_of[7], 71), 0)
    diag_upper_inv = draw_diag_upper_inv(jax.random.fold_in(key_of[7], 71), 0)
    return {"trailing": trailing, "col_u": col_u, "col_v": col_v, "row_u": row_u, "row_v": row_v, "diag_lower_inv": diag_lower_inv, "diag_upper_inv": diag_upper_inv}


def reference(trailing, col_u, col_v, row_u, row_v, diag_lower_inv, diag_upper_inv):
    highest = lax.Precision.HIGHEST
    left_v = jnp.einsum("ba,tbr->tar", diag_upper_inv, col_v.astype(jnp.float32), precision=highest)
    lower = jnp.einsum("tpr,tar->tpa", col_u.astype(jnp.float32), left_v, precision=highest).astype(jnp.bfloat16)
    right_u = jnp.einsum("ab,tbr->tar", diag_lower_inv, row_u.astype(jnp.float32), precision=highest)
    upper = jnp.einsum("tar,tqr->taq", right_u, row_v.astype(jnp.float32), precision=highest).astype(jnp.bfloat16)
    upper_whole = jnp.transpose(upper, (1, 0, 2)).reshape(B, NT * B)

    def update(pair):
        rows, tile = pair
        product = jnp.dot(tile, upper_whole, preferred_element_type=jnp.float32)
        return (rows.astype(jnp.float32) - product).astype(jnp.bfloat16)

    blocks = lax.map(update, (trailing.reshape(MT, B, NT * B), lower))
    return blocks.reshape(MT * B, NT * B)
```

```python
import functools

import jax
import jax.numpy as jnp
from jax import lax
from jax.experimental import pallas as pl
from jax.experimental.pallas import tpu as pltpu
from jax.sharding import PartitionSpec as P

MESH = pl.DeviceIdType.MESH
F32 = jnp.float32
BF16 = jnp.bfloat16


def partner(at, step, count):
    if count & (count - 1):
        return lax.rem(at + step, count)
    out = jnp.int32(0)
    weight = 1
    while weight < count:
        bit = (at // weight) % 2
        out = out + weight * ((1 - bit) if step & weight else bit)
        weight *= 2
    return out


def source(at, step, count):
    if count & (count - 1):
        return lax.rem(at + count - step, count)
    return partner(at, step, count)


def split(x):
    high = x.astype(BF16)
    return high, (x - high.astype(F32)).astype(BF16)


def dot(a, b):
    return lax.dot_general(a, b, (((1,), (0,)), ((), ())), preferred_element_type=F32)


def dot_rt(a, b):
    return lax.dot_general(a, b, (((1,), (1,)), ((), ())), preferred_element_type=F32)


def pack(left, right):
    return jnp.concatenate([left.astype(F32), right.astype(F32)], axis=-1).astype(BF16)


def panel_kernel(
    n_row, n_col,
    cu_hbm, cv_hbm, ru_hbm, rv_hbm, dl_hbm, du_hbm, trail_hbm,
    out_ref,
    ru, rv, dl, du, trail, mh, ml, cuall, cvall, gall,
    in_sem, cu_send, cu_recv, cv_send, cv_recv, row_send, row_recv, fwd_send,
):
    row = lax.axis_index("row")
    col = lax.axis_index("col")
    paired = n_row % 2 == 0
    width = 2 if paired else 1
    chips = n_row // width
    core = row % width
    chip = row // width

    col_steps = list(range(n_col - 1, 0, -1))
    chip_steps = list(range(chips - 1, 0, -1))
    col_to = {k: partner(col, k, n_col) for k in col_steps}
    col_from = {k: source(col, k, n_col) for k in col_steps}
    row_to = {k: partner(chip, k, chips) * width + core for k in chip_steps}
    row_from = {k: source(chip, k, chips) * width + core for k in chip_steps}
    mate = chip * width + (1 - core) if paired else row

    barrier = pltpu.get_barrier_semaphore()
    peers = [(row, col_to[k]) for k in col_steps] + [(row_to[k], col) for k in chip_steps]
    if paired:
        peers.append((mate, col))
    for peer in peers:
        pl.semaphore_signal(barrier, inc=1, device_id=peer, device_id_type=MESH)

    loads = []
    for n, (src, dst) in enumerate([
        (ru_hbm, ru), (rv_hbm, rv), (cv_hbm, cvall.at[col]), (cu_hbm, cuall.at[col]),
        (dl_hbm, dl), (du_hbm, du), (trail_hbm, trail),
    ]):
        load = pltpu.make_async_copy(src, dst, in_sem.at[n])
        load.start()
        loads.append(load)

    loads[0].wait()
    loads[1].wait()
    gall[row] = pack(ru[...], rv[...])
    loads[2].wait()
    loads[3].wait()

    pl.semaphore_wait(barrier, len(peers))

    def row_copy(slot, send_sem, to):
        return pltpu.make_async_remote_copy(
            src_ref=gall.at[slot], dst_ref=gall.at[slot], send_sem=send_sem,
            recv_sem=row_recv.at[slot], device_id=(to, col), device_id_type=MESH,
        )

    def col_copy(slots, recv, slot, send_sem, to):
        return pltpu.make_async_remote_copy(
            src_ref=slots.at[slot], dst_ref=slots.at[slot], send_sem=send_sem,
            recv_sem=recv.at[slot], device_id=(row, to), device_id_type=MESH,
        )

    sends = []
    for k in chip_steps:
        sends.append(row_copy(row, row_send.at[k], row_to[k]))
        sends[-1].start()
    for k in col_steps:
        sends.append(col_copy(cvall, cv_recv, col, cv_send.at[k], col_to[k]))
        sends[-1].start()
    for k in col_steps:
        sends.append(col_copy(cuall, cu_recv, col, cu_send.at[k], col_to[k]))
        sends[-1].start()
    if paired:
        sends.append(row_copy(row, row_send.at[0], mate))
        sends[-1].start()

    loads[4].wait()
    loads[5].wait()
    order = dl.shape[0]
    half = order // 2
    uh, ul = split(du[...])
    lh, ll = split(dl[...])

    def product(rows, mid, cols):
        a, b = uh[rows, mid], ul[rows, mid]
        c, d = lh[mid, cols], ll[mid, cols]
        return dot(a, c) + (dot(a, d) + dot(b, c))

    lo, hi, full = slice(0, half), slice(half, order), slice(0, order)
    for rows, mid, cols in ((lo, full, lo), (lo, hi, hi), (hi, hi, lo), (hi, hi, hi)):
        mh[rows, cols], ml[rows, cols] = split(product(rows, mid, cols))

    tiles, rank = cvall.shape[1], cvall.shape[2]
    for k in reversed(col_steps):
        col_copy(cvall, cv_recv, col_from[k], cv_send.at[k], col_to[k]).wait_recv()
    weights = []
    for t in range(tiles):
        turned = jnp.concatenate([cvall[c, t] for c in range(n_col)], axis=-1)
        wh, wl = split(dot(turned, mh[...]) + dot(turned, ml[...]))
        weights.append(jnp.concatenate([wh, wl], axis=0))

    for k in reversed(col_steps):
        col_copy(cuall, cu_recv, col_from[k], cu_send.at[k], col_to[k]).wait_recv()
    lefts = []
    for t in range(tiles):
        turned = jnp.concatenate([cuall[c, t] for c in range(n_col)], axis=-1).astype(F32)
        lefts.append(jnp.concatenate([turned, turned], axis=0).T.astype(BF16))

    for k in reversed(chip_steps):
        slot = row_from[k]
        row_copy(slot, row_send.at[k], row_to[k]).wait_recv()
        if paired:
            sends.append(row_copy(slot, fwd_send.at[k], mate))
            sends[-1].start()
    if paired:
        row_copy(mate, row_send.at[0], mate).wait_recv()
        for k in reversed(chip_steps):
            slot = source(chip, k, chips) * width + (1 - core)
            row_copy(slot, fwd_send.at[k], mate).wait_recv()
    loads[6].wait()

    for j in range(gall.shape[1]):
        g = gall[:, j].reshape(order, 2 * rank)
        at = pl.ds(j * order, order)
        for t in range(tiles):
            c = dot(weights[t], g)
            c = c[:rank, :rank] + c[rank:, :rank]
            ch, cl = split(jnp.concatenate([jnp.zeros_like(c), c], axis=-1))
            right = dot_rt(jnp.concatenate([ch, cl], axis=0), g)
            th, tl = split(right[:rank] + right[rank:])
            update = dot(lefts[t], jnp.concatenate([th, tl], axis=0))
            rows = pl.ds(t * order, order)
            out_ref[rows, at] = (trail[rows, at].astype(F32) - update).astype(BF16)

    for send in sends:
        send.wait_send()


def shards(n_row, n_col, trailing, col_u, col_v, row_u, row_v, diag_lower_inv, diag_upper_inv):
    mt, cc, rank = col_u.shape
    nt, rc, _ = row_u.shape
    order = diag_lower_inv.shape[0]
    anywhere = pl.BlockSpec(memory_space=pl.ANY)
    dma = pltpu.SemaphoreType.DMA
    return pl.pallas_call(
        functools.partial(panel_kernel, n_row, n_col),
        out_shape=pltpu.VMEM(trailing.shape, BF16),
        in_specs=[anywhere] * 7,
        out_specs=pl.BlockSpec(memory_space=pltpu.VMEM),
        scratch_shapes=[
            pltpu.VMEM(row_u.shape, BF16),
            pltpu.VMEM(row_v.shape, BF16),
            pltpu.VMEM((order, order), F32),
            pltpu.VMEM((order, order), F32),
            pltpu.VMEM(trailing.shape, BF16),
            pltpu.VMEM((order, order), BF16),
            pltpu.VMEM((order, order), BF16),
            pltpu.VMEM((n_col, mt, rank, cc), BF16),
            pltpu.VMEM((n_col, mt, rank, cc), BF16),
            pltpu.VMEM((n_row, nt, rc, 2 * rank), BF16),
            dma((7,)), dma((n_col,)), dma((n_col,)), dma((n_col,)), dma((n_col,)),
            dma((n_row,)), dma((n_row,)), dma((n_row,)),
        ],
        compiler_params=pltpu.CompilerParams(collective_id=0, has_side_effects=True),
        name="panels",
    )(
        jnp.swapaxes(col_u, 1, 2), jnp.swapaxes(col_v, 1, 2), row_u, row_v,
        diag_lower_inv, diag_upper_inv, trailing,
    )


def solution(mesh):
    placed = (
        P("row", "col"),
        P("row", "col", None),
        P("row", "col", None),
        P("col", "row", None),
        P("col", "row", None),
        P(),
        P(),
    )
    return jax.shard_map(
        functools.partial(shards, mesh.shape["row"], mesh.shape["col"]),
        mesh=mesh, in_specs=placed, out_specs=P("row", "col"), check_vma=False,
    )
```

```python
import functools

import jax
import jax.numpy as jnp
from jax import lax
from jax.experimental import pallas as pl
from jax.experimental.pallas import tpu as pltpu
from jax.sharding import PartitionSpec as P

MESH = pl.DeviceIdType.MESH
F32 = jnp.float32
BF16 = jnp.bfloat16
BLOCKS = 1


def partner(at, step, count):
    if count & (count - 1):
        return lax.rem(at + step, count)
    out = jnp.int32(0)
    weight = 1
    while weight < count:
        bit = (at // weight) % 2
        out = out + weight * ((1 - bit) if step & weight else bit)
        weight *= 2
    return out


def source(at, step, count):
    if count & (count - 1):
        return lax.rem(at + count - step, count)
    return partner(at, step, count)


def split(x):
    high = x.astype(BF16)
    return high, (x - high.astype(F32)).astype(BF16)


def dot(a, b):
    return lax.dot_general(a, b, (((1,), (0,)), ((), ())), preferred_element_type=F32)


def dot_rt(a, b):
    return lax.dot_general(a, b, (((1,), (1,)), ((), ())), preferred_element_type=F32)


def pack(left, right):
    return jnp.concatenate([left.astype(F32), right.astype(F32)], axis=-1).astype(BF16)


def panel_kernel(
    n_row, n_col,
    cu_hbm, cv_hbm, ru_hbm, rv_hbm, dl_hbm, du_hbm, trail_hbm,
    t_ref, cu_ref, trail,
    ru, rv, dl, du, mh, ml, cuall, cvall, gall,
    in_sem, cu_send, cu_recv, cv_send, cv_recv, row_send, row_recv, fwd_send,
):
    row = lax.axis_index("row")
    col = lax.axis_index("col")
    paired = n_row % 2 == 0
    width = 2 if paired else 1
    chips = n_row // width
    core = row % width
    chip = row // width

    col_steps = list(range(n_col - 1, 0, -1))
    chip_steps = list(range(chips - 1, 0, -1))
    col_to = {k: partner(col, k, n_col) for k in col_steps}
    col_from = {k: source(col, k, n_col) for k in col_steps}
    row_to = {k: partner(chip, k, chips) * width + core for k in chip_steps}
    row_from = {k: source(chip, k, chips) * width + core for k in chip_steps}
    mate = chip * width + (1 - core) if paired else row

    barrier = pltpu.get_barrier_semaphore()
    peers = [(row, col_to[k]) for k in col_steps] + [(row_to[k], col) for k in chip_steps]
    if paired:
        peers.append((mate, col))
    for peer in peers:
        pl.semaphore_signal(barrier, inc=1, device_id=peer, device_id_type=MESH)

    loads = []
    for n, (src, dst) in enumerate([
        (ru_hbm, ru), (rv_hbm, rv), (cv_hbm, cvall.at[col]), (cu_hbm, cuall.at[col]),
        (dl_hbm, dl), (du_hbm, du), (trail_hbm, trail),
    ]):
        load = pltpu.make_async_copy(src, dst, in_sem.at[n])
        load.start()
        loads.append(load)

    loads[0].wait()
    loads[1].wait()
    gall[row] = pack(ru[...], rv[...])
    loads[2].wait()
    loads[3].wait()

    pl.semaphore_wait(barrier, len(peers))

    def row_copy(slot, send_sem, to):
        return pltpu.make_async_remote_copy(
            src_ref=gall.at[slot], dst_ref=gall.at[slot], send_sem=send_sem,
            recv_sem=row_recv.at[slot], device_id=(to, col), device_id_type=MESH,
        )

    def col_copy(slots, recv, slot, send_sem, to):
        return pltpu.make_async_remote_copy(
            src_ref=slots.at[slot], dst_ref=slots.at[slot], send_sem=send_sem,
            recv_sem=recv.at[slot], device_id=(row, to), device_id_type=MESH,
        )

    sends = []
    for k in chip_steps:
        sends.append(row_copy(row, row_send.at[k], row_to[k]))
        sends[-1].start()
    for k in col_steps:
        sends.append(col_copy(cvall, cv_recv, col, cv_send.at[k], col_to[k]))
        sends[-1].start()
    for k in col_steps:
        sends.append(col_copy(cuall, cu_recv, col, cu_send.at[k], col_to[k]))
        sends[-1].start()
    if paired:
        sends.append(row_copy(row, row_send.at[0], mate))
        sends[-1].start()

    loads[4].wait()
    loads[5].wait()
    order = dl.shape[0]
    half = order // 2
    uh, ul = split(du[...])
    lh, ll = split(dl[...])

    def product(rows, mid, cols):
        a, b = uh[rows, mid], ul[rows, mid]
        c, d = lh[mid, cols], ll[mid, cols]
        return dot(a, c) + (dot(a, d) + dot(b, c))

    lo, hi, full = slice(0, half), slice(half, order), slice(0, order)
    for rows, mid, cols in ((lo, full, lo), (lo, hi, hi), (hi, hi, lo), (hi, hi, hi)):
        mh[rows, cols], ml[rows, cols] = split(product(rows, mid, cols))

    for k in reversed(chip_steps):
        slot = row_from[k]
        row_copy(slot, row_send.at[k], row_to[k]).wait_recv()
        if paired:
            sends.append(row_copy(slot, fwd_send.at[k], mate))
            sends[-1].start()

    tiles, rank = cvall.shape[1], cvall.shape[2]
    for k in reversed(col_steps):
        col_copy(cvall, cv_recv, col_from[k], cv_send.at[k], col_to[k]).wait_recv()
    weights = []
    for t in range(tiles):
        turned = jnp.concatenate([cvall[c, t] for c in range(n_col)], axis=-1)
        wh, wl = split(dot(turned, mh[...]) + dot(turned, ml[...]))
        weights.append(jnp.concatenate([wh, wl], axis=0))

    for k in reversed(col_steps):
        col_copy(cuall, cu_recv, col_from[k], cu_send.at[k], col_to[k]).wait_recv()
    lefts = []
    for t in range(tiles):
        turned = jnp.concatenate([cuall[c, t] for c in range(n_col)], axis=-1).astype(F32)
        lefts.append(jnp.concatenate([turned, turned], axis=0).T.astype(BF16))

    if paired:
        row_copy(mate, row_send.at[0], mate).wait_recv()
        for k in reversed(chip_steps):
            slot = source(chip, k, chips) * width + (1 - core)
            row_copy(slot, fwd_send.at[k], mate).wait_recv()
    loads[6].wait()

    panels = [gall[:, j].reshape(order, 2 * rank) for j in range(gall.shape[1])]
    spread = jnp.concatenate(panels, axis=-1)
    for t in range(tiles):
        c = dot(weights[t], spread)
        c = c[:rank] + c[rank:]
        rights = []
        for j, g in enumerate(panels):
            core_j = c[:, 2 * rank * j:2 * rank * j + rank]
            ch, cl = split(jnp.concatenate([jnp.zeros_like(core_j), core_j], axis=-1))
            right = dot_rt(jnp.concatenate([ch, cl], axis=0), g)
            th, tl = split(right[:rank] + right[rank:])
            rights.append(jnp.concatenate([th, tl], axis=0))
        cu_ref[t] = lefts[t]
        for j, right in enumerate(rights):
            t_ref[t, :, pl.ds(j * order, order)] = right

    for send in sends:
        send.wait_send()


def update_kernel(blocks, t_ref, cu_ref, trail, out_hbm, out, out_sem):
    tiles, order, _ = cu_ref.shape
    wide = t_ref.shape[2] // blocks
    copies = []
    for t in range(tiles):
        rows = pl.ds(t * order, order)
        for b in range(blocks):
            at = pl.ds(b * wide, wide)
            product = dot(cu_ref[t], t_ref[t, :, at])
            out[rows, at] = (trail[rows, at].astype(F32) - product).astype(BF16)
            copy = pltpu.make_async_copy(out.at[rows, at], out_hbm.at[rows, at], out_sem.at[t * blocks + b])
            copy.start()
            copies.append(copy)
    for copy in copies:
        copy.wait()


def shards(n_row, n_col, trailing, col_u, col_v, row_u, row_v, diag_lower_inv, diag_upper_inv):
    mt, cc, rank = col_u.shape
    nt, rc, _ = row_u.shape
    order = diag_lower_inv.shape[0]
    anywhere = pl.BlockSpec(memory_space=pl.ANY)
    dma = pltpu.SemaphoreType.DMA
    wide = nt * order
    vmem = pl.BlockSpec(memory_space=pltpu.VMEM)
    handed = pl.pallas_call(
        functools.partial(panel_kernel, n_row, n_col),
        out_shape=[
            pltpu.VMEM((mt, 2 * rank, wide), BF16),
            pltpu.VMEM((mt, order, 2 * rank), BF16),
            pltpu.VMEM(trailing.shape, BF16),
        ],
        in_specs=[anywhere] * 7,
        out_specs=[vmem] * 3,
        scratch_shapes=[
            pltpu.VMEM(row_u.shape, BF16),
            pltpu.VMEM(row_v.shape, BF16),
            pltpu.VMEM((order, order), F32),
            pltpu.VMEM((order, order), F32),
            pltpu.VMEM((order, order), BF16),
            pltpu.VMEM((order, order), BF16),
            pltpu.VMEM((n_col, mt, rank, cc), BF16),
            pltpu.VMEM((n_col, mt, rank, cc), BF16),
            pltpu.VMEM((n_row, nt, rc, 2 * rank), BF16),
            dma((7,)), dma((n_col,)), dma((n_col,)), dma((n_col,)), dma((n_col,)),
            dma((n_row,)), dma((n_row,)), dma((n_row,)),
        ],
        compiler_params=pltpu.CompilerParams(collective_id=0, has_side_effects=True),
        name="panels",
    )(
        jnp.swapaxes(col_u, 1, 2), jnp.swapaxes(col_v, 1, 2), row_u, row_v,
        diag_lower_inv, diag_upper_inv, trailing,
    )
    handed = [pltpu.with_memory_space_constraint(x, pltpu.VMEM) for x in handed]
    blocks = BLOCKS * nt
    return pl.pallas_call(
        functools.partial(update_kernel, blocks),
        out_shape=jax.ShapeDtypeStruct(trailing.shape, BF16),
        in_specs=[vmem] * 3,
        out_specs=anywhere,
        scratch_shapes=[pltpu.VMEM(trailing.shape, BF16), dma((mt * blocks,))],
        name="update",
    )(*handed)


def solution(mesh):
    placed = (
        P("row", "col"),
        P("row", "col", None),
        P("row", "col", None),
        P("col", "row", None),
        P("col", "row", None),
        P(),
        P(),
    )
    return jax.shard_map(
        functools.partial(shards, mesh.shape["row"], mesh.shape["col"]),
        mesh=mesh, in_specs=placed, out_specs=P("row", "col"), check_vma=False,
    )
```
